256 devices in a mesh: cuts: 4 (over x, y), ma: 32 (over z), mb: 2 (over core).
Axes of the slice: x: 2, y: 2, z: 32, core: 2. Of those that a mesh axis runs over, the one named last changes fastest.
The devices are a block of a 4x8x32 slice.
Arguments:
- stem_field: bfloat16 [512, 512, 2, 512], P(('cuts', 'ma', 'mb')), parts along dimension 0, may hold values from -6 to 6
- first_branch_tensors: bfloat16 [2, 2, 512, 512], P(None, None, 'ma'), may hold values from -0.1875 to 0.1875
- second_branch_tensors: bfloat16 [2, 2, 512, 512], P(None, None, 'ma'), may hold values from -0.1875 to 0.1875
- relabel: int32 [2, 512], replicated, may hold values from 0 to 511, each once within a row
- sample_block: int32 [65536, 1], P(('cuts', 'ma', 'mb')), parts along dimension 0, may hold values from 0 to 127; in each aligned block of 256 rows (0 to 255, 256 to 511, ...) at most 4 rows name the same one
- sample_state: bfloat16 [65536, 2, 512], P(('cuts', 'ma', 'mb')), parts along dimension 0, may hold values from -0.1875 to 0.1875
Outputs:
- amplitudes: bfloat16 [65536, 2, 512], P(('cuts', 'ma', 'mb')), parts along dimension 0
The draws below stay inside these ranges and needn't reach their ends.
There are 4 independent parts, one for each index of `cuts`. The reference program is written for one: setup_inputs(seed, part) draws one part's arguments, and reference() takes and returns one part's arrays. A program takes and returns all parts, laid end to end along the dimension named above; an argument that names none is the same for every part. Nothing has to cross between parts.
Inputs may be any that keep to these rules, and one draw needn't show every extreme that they name: `relabel`: each row is a permutation of 0 to 511. `sample_block`: within the 256 rows of one device no prefix block is named more than 4 times.
All inputs are finite; a program needn't handle non-finite values.
Results may differ from the reference program's by a relative error of at most 0.0075.
Values may be sent and summed in bfloat16 or wider, within the bound.
A program may use at most 64 MiB of HBM per device.

```python
import math
import jax
import jax.numpy as jnp
import numpy as np
from jax import lax

FIRST_MODE_SIZE = 512
SECOND_MODE_SIZE = 512
REGROUP_COUNT = 2
SAMPLES_DEVICE = 256
S = 128
SAMP = 16384
MOST = 4
N_MA = 32
N_MB = 2


def level_of(key, extent, split, least, high):
    def one(dim, blocks):
        heights = jax.random.uniform(jax.random.fold_in(jax.random.fold_in(key, 6), dim), (blocks,), jnp.float32, least / len(split), high / len(split))
        return jnp.repeat(jnp.exp(heights), extent[dim] // blocks).reshape((-1,) + (1,) * (len(extent) - dim - 1))

    level = one(*split[0])
    for cut in split[1:]:
        level = level * one(*cut)
    return level


def shared_out(key, own, number, rows, amount, top, most, lean):
    ranking = jax.random.permutation(key, amount)
    crowded, ordinary = load_shares(amount, rows * top, most, lean, True), load_shares(amount, rows * top, most, lean, False)
    places = jnp.arange(amount)

    def named(lengths, offset_by):
        used = int((lengths > 0).sum())
        fixed = max(1, used // 4)
        passed = fixed + (places - fixed + offset_by * (used - fixed)) % max(1, amount - fixed)
        return jnp.zeros((amount,), jnp.int32).at[ranking[jnp.where(places < fixed, places, passed)]].set(jnp.asarray(lengths, jnp.int32))

    lengths = jnp.where(number % 4 == 0, named(crowded, number // 4), named(ordinary, number - number // 4 - 1))
    mixed = jax.random.permutation(jax.random.fold_in(own, 3), amount)
    source_of, sink = mixed[0:amount // 2 * 2:2], mixed[1:amount // 2 * 2:2]
    slack = jnp.minimum(lengths[source_of] - 1, most - lengths[sink]) // 2
    slack = jnp.where((source_of == ranking[0]) | (sink == ranking[0]) | (lengths[sink] == 0), 0, jnp.maximum(slack, 0))
    passed = jax.random.randint(jax.random.fold_in(own, 4), (amount // 2,), 0, 1 << 20) % (slack + 1)
    lengths = lengths.at[source_of].add(-passed).at[sink].add(passed)
    labels = jnp.searchsorted(jnp.cumsum(lengths), jnp.arange(rows * top), side="right").astype(jnp.int32)
    grid = labels.reshape(top, rows).T
    grid = grid[jax.random.permutation(jax.random.fold_in(own, 1), rows)]
    offset_by = jax.random.randint(jax.random.fold_in(own, 2), (rows, 1), 0, top)
    return jnp.take_along_axis(grid, (jnp.arange(top)[None, :] + offset_by) % top, axis=1)


def load_shares(count, total, most, lean, full):
    weights = [(1 << 20) // math.isqrt(grade ** lean) + 1 for grade in range(1, count + 1)]
    largest = most if full else min(most, max(-(-total // count), total * weights[0] // sum(weights)))
    least = 1 if total - largest >= count - 1 else 0
    given, spare = [largest] + [least] * (count - 1), total - largest - least * (count - 1)
    while spare > 0:
        candidates = [i for i in range(1, count) if given[i] < largest] or [i for i in range(1, count) if given[i] < most]
        mass, budget = sum([weights[i] for i in candidates]), spare
        for i in candidates:
            extra = min(most - given[i], max(1, budget * weights[i] // mass), spare)
            given[i] = given[i] + extra
            spare = spare - extra
    return np.array(given)


def gaussian(own_key, dims, width, limit, cuts=(), held_as=jnp.bfloat16):
    values = jax.random.normal(own_key, dims, jnp.float32) * width
    if len(cuts) > 0:
        values = level_of(own_key, dims, cuts, -0.22, 0.18) * values
    return jnp.clip(values, min=-limit, max=limit).astype(held_as)


def setup_inputs(seed: int = 0, part: int = 0) -> dict:
    keys = jax.random.split(jax.random.key(seed), 7)
    part_keys = jax.random.split(jax.random.fold_in(keys[6], part), 7)
    stem_field = gaussian(part_keys[0], (S, FIRST_MODE_SIZE, 2, SECOND_MODE_SIZE), 1.0, 6.0, ((0, 64),))
    first_branch_tensors = gaussian(keys[1], (REGROUP_COUNT, 2, FIRST_MODE_SIZE, FIRST_MODE_SIZE), (2 * FIRST_MODE_SIZE) ** -0.5, 0.1875, ((2, 32),))
    second_branch_tensors = gaussian(keys[2], (REGROUP_COUNT, 2, SECOND_MODE_SIZE, SECOND_MODE_SIZE), (2 * SECOND_MODE_SIZE) ** -0.5, 0.1875, ((2, 32),))
    relabel = jax.vmap(lambda own: jax.random.permutation(own, FIRST_MODE_SIZE))(jax.random.split(keys[3], REGROUP_COUNT)).reshape((REGROUP_COUNT, FIRST_MODE_SIZE)).astype(jnp.int32)
    sample_block_keys = jax.random.split(jax.random.fold_in(part_keys[4], 1), SAMP // SAMPLES_DEVICE)
    sample_block_turns = jax.random.permutation(jax.random.fold_in(part_keys[4], 3), SAMP // SAMPLES_DEVICE)
    sample_block = jax.vmap(lambda own, number: shared_out(jax.random.fold_in(part_keys[4], 2), own, number, SAMPLES_DEVICE, S, 1, MOST, 2))(sample_block_keys, sample_block_turns).reshape((SAMP, 1))
    sample_state = gaussian(part_keys[5], (SAMP, 2, SECOND_MODE_SIZE), (2 * SECOND_MODE_SIZE) ** -0.5, 0.1875, ((0, 64),))
    return {"stem_field": stem_field, "first_branch_tensors": first_branch_tensors, "second_branch_tensors": second_branch_tensors, "relabel": relabel, "sample_block": sample_block, "sample_state": sample_state}


def regroup(stem_field, groups):
    blocks, row_count, part_count, col_count = stem_field.shape
    local_blocks = blocks // groups
    pieces = stem_field.reshape(groups, local_blocks, groups, row_count // groups, part_count, col_count)
    pieces = jnp.transpose(pieces, (2, 1, 0, 3, 4, 5))
    return pieces.reshape(blocks, row_count, part_count, col_count)


def complex_contract(stem_field, matrix, pattern):
    real_part = stem_field[:, :, 0, :].astype(jnp.float32)
    imag_part = stem_field[:, :, 1, :].astype(jnp.float32)
    matrix_real = matrix[0].astype(jnp.float32)
    matrix_imag = matrix[1].astype(jnp.float32)

    def product(operand, table):
        return jnp.einsum(pattern, operand, table, precision=lax.Precision.HIGHEST)

    out_real = product(real_part, matrix_real) - product(imag_part, matrix_imag)
    out_imag = product(real_part, matrix_imag) + product(imag_part, matrix_real)
    return jnp.stack([out_real, out_imag], axis=2).astype(jnp.bfloat16)


def reference(stem_field, first_branch_tensors, second_branch_tensors, relabel, sample_block, sample_state):
    groups = N_MA * N_MB
    for regroup_round_index in range(REGROUP_COUNT):
        stem_field = regroup(stem_field, groups)
        stem_field = jnp.take(stem_field, relabel[regroup_round_index].astype(jnp.int32), axis=1)
        stem_field = complex_contract(stem_field, first_branch_tensors[regroup_round_index], "sab,ao->sob")
        stem_field = complex_contract(stem_field, second_branch_tensors[regroup_round_index], "sab,bo->sao")
    batch_size = 32
    owners = sample_block[:, 0].astype(jnp.int32).reshape(-1, batch_size)
    states = sample_state.reshape(-1, batch_size, 2, sample_state.shape[2])

    def evaluate(pair):
        indices, batch_states = pair
        chosen = jnp.take(stem_field, indices, axis=0).astype(jnp.float32)
        state_real = batch_states[:, 0].astype(jnp.float32)
        state_imag = batch_states[:, 1].astype(jnp.float32)

        def product(operand, vector):
            return jnp.einsum("nab,nb->na", operand, vector, precision=lax.Precision.HIGHEST)

        out_real = product(chosen[:, :, 0], state_real) - product(chosen[:, :, 1], state_imag)
        out_imag = product(chosen[:, :, 0], state_imag) + product(chosen[:, :, 1], state_real)
        return jnp.stack([out_real, out_imag], axis=1).astype(jnp.bfloat16)

    amplitudes = lax.map(evaluate, (owners, states))
    return amplitudes.reshape(sample_state.shape[0], 2, stem_field.shape[1])
```

```python
import functools

import jax
import jax.numpy as jnp
from jax import lax
from jax.experimental import pallas as pl
from jax.experimental.pallas import tpu as pltpu
from jax.sharding import PartitionSpec as P

LANES = 128
TILE = 16
MESH = pl.DeviceIdType.MESH


def complex_table(matrix):
    real_part, imag_part = matrix[0], matrix[1]
    upper_rows = jnp.stack([real_part, imag_part], axis=1)
    lower_rows = jnp.stack([-imag_part, real_part], axis=1)
    rows, width = real_part.shape
    return jnp.stack([upper_rows, lower_rows], axis=0).reshape(2 * rows, 2 * width)


def ring_kernel(
    ring,
    mode_rows,
    kept_from,
    states_ref,
    stem_ref,
    table_ref,
    out_ref,
    states,
    sums,
    kept,
    stems,
    wide,
    products,
    coef,
    local_sem,
    stem_sem,
    state_send,
    state_recv,
    sum_send,
    sum_recv,
):
    me = lax.axis_index("ma")
    core = lax.axis_index("mb")
    right, left = lax.rem(me + 1, ring), lax.rem(me + ring - 1, ring)
    other_core = 1 - core
    last = ring

    barrier = pltpu.get_barrier_semaphore()
    pl.semaphore_signal(barrier, inc=1, device_id={"ma": right}, device_id_type=MESH)
    pl.semaphore_signal(barrier, inc=1, device_id={"ma": left}, device_id_type=MESH)
    pl.semaphore_signal(barrier, inc=1, device_id={"mb": other_core}, device_id_type=MESH)

    own_states = [
        pltpu.make_async_copy(
            states_ref.at[d if j == 0 else 1 - d], states.at[j, d], local_sem.at[2 * j + d]
        )
        for j in range(2)
        for d in range(2)
    ]
    own_stem = pltpu.make_async_copy(stem_ref, stems.at[0], local_sem.at[4])
    for copy in own_states:
        copy.start()
    own_stem.start()
    pl.semaphore_wait(barrier, 3)
    swap = pltpu.make_async_remote_copy(
        src_ref=stem_ref,
        dst_ref=stems.at[1],
        send_sem=stem_sem.at[0],
        recv_sem=stem_sem.at[1],
        device_id={"mb": other_core},
        device_id_type=MESH,
    )
    swap.start()
    for copy in own_states:
        copy.wait()

    def state_copy(d, j):
        return pltpu.make_async_remote_copy(
            src_ref=states.at[j, d],
            dst_ref=states.at[j + 2, d],
            send_sem=state_send.at[j, d],
            recv_sem=state_recv.at[j, d],
            device_id={"ma": (right, left)[d]},
            device_id_type=MESH,
        )

    def sum_copy(d, j):
        return pltpu.make_async_remote_copy(
            src_ref=sums.at[j, d],
            dst_ref=sums.at[j - 2, d],
            send_sem=sum_send.at[j - 2, d],
            recv_sem=sum_recv.at[j - 2, d],
            device_id={"ma": (left, right)[d]},
            device_id_type=MESH,
        )

    tiles = stems.shape[1]
    depth = stems.shape[3]
    half = depth // 2
    blocks = table_ref.shape[1]
    parity_row = 4 * mode_rows * mode_rows
    out_half = tiles * mode_rows * TILE

    def contribution(j, slot):
        def one(d, carry):
            real_part = states[j, d, 0:half, :]
            imag_part = states[j, d, half:depth, :]
            wide[0:half, 0:LANES] = real_part
            wide[0:half, LANES : 2 * LANES] = imag_part
            wide[half:depth, 0:LANES] = -imag_part
            wide[half:depth, LANES : 2 * LANES] = real_part
            named = states[j, d, depth : depth + TILE, :].astype(jnp.float32)[0:1, :]
            counted = lax.broadcasted_iota(jnp.int32, (blocks, LANES), 0).astype(jnp.float32)
            hot = jnp.where(counted == named, 1.0, 0.0).astype(jnp.bfloat16)
            coef[...] = jnp.dot(table_ref[...], hot, preferred_element_type=jnp.float32)

            def tile_step(t, carry):
                for h in range(2):
                    products[h] = jnp.dot(
                        stems[h, t], wide[...], preferred_element_type=jnp.float32
                    )
                odd = jnp.broadcast_to(coef[parity_row : parity_row + 1, :], (TILE, LANES)) > 0.5
                sum_real = [jnp.zeros((TILE, LANES), jnp.float32)] * mode_rows
                sum_imag = [jnp.zeros((TILE, LANES), jnp.float32)] * mode_rows
                for h in range(2):
                    for r in range(mode_rows):
                        even_rows = pl.ds(r * TILE, TILE)
                        odd_rows = pl.ds((mode_rows + r) * TILE, TILE)
                        y_real = jnp.where(
                            odd, products[h, odd_rows, 0:LANES], products[h, even_rows, 0:LANES]
                        )
                        y_imag = jnp.where(
                            odd,
                            products[h, odd_rows, LANES : 2 * LANES],
                            products[h, even_rows, LANES : 2 * LANES],
                        )
                        for q in range(mode_rows):
                            row = ((h * mode_rows + r) * 2) * mode_rows + q
                            c_real = jnp.broadcast_to(coef[row : row + 1, :], (TILE, LANES))
                            row = row + mode_rows
                            c_imag = jnp.broadcast_to(coef[row : row + 1, :], (TILE, LANES))
                            sum_real[q] = sum_real[q] + (c_real * y_real - c_imag * y_imag)
                            sum_imag[q] = sum_imag[q] + (c_real * y_imag + c_imag * y_real)
                for q in range(mode_rows):
                    start = pl.multiple_of(t * (mode_rows * TILE), TILE) + q * TILE
                    kept[slot, d, pl.ds(start, TILE), :] = sum_real[q]
                    kept[slot, d, pl.ds(out_half + start, TILE), :] = sum_imag[q]
                return carry

            return lax.fori_loop(0, tiles, tile_step, carry)

        lax.fori_loop(0, 2, one, 0)

    def spread(j, carry):
        @pl.when(j >= 2)
        def _():
            for d in range(2):
                state_copy(d, j - 2).wait_recv()

        @pl.when(j <= last - 2)
        def _():
            for d in range(2):
                state_copy(d, j).start()

        @pl.when(j == kept_from)
        def _():
            own_stem.wait()
            swap.wait()

        @pl.when(j >= kept_from)
        def _():
            contribution(j, j - kept_from)

        @pl.when(j >= last - 1)
        def _():
            for d in range(2):
                sums[j, d] = kept[j - kept_from, d].astype(jnp.bfloat16)
                sum_copy(d, j).start()

        return carry

    lax.fori_loop(0, last + 1, spread, 0)
    spare = last - kept_from

    def collect(i, carry):
        j = last - 2 - i

        @pl.when(jnp.logical_and(j < kept_from, j != 1))
        def _():
            contribution(j, spare)

        for d in range(2):
            sum_copy(d, j + 2).wait_recv()

            @pl.when(jnp.logical_and(j >= 2, j < kept_from))
            def _():
                sums[j, d] = (sums[j, d].astype(jnp.float32) + kept[spare, d]).astype(jnp.bfloat16)

            @pl.when(j >= kept_from)
            def _():
                sums[j, d] = (
                    sums[j, d].astype(jnp.float32) + kept[j - kept_from, d]
                ).astype(jnp.bfloat16)

            @pl.when(j >= 2)
            def _():
                sum_copy(d, j).start()

        return carry

    lax.fori_loop(0, last - 1, collect, 0)
    for d in range(2):
        out_ref[d] = (
            sums[0, d].astype(jnp.float32) + sums[1, 1 - d].astype(jnp.float32) + kept[spare, d]
        )

    def drain(j, carry):
        for d in range(2):
            state_copy(d, j).wait_send()
            sum_copy(d, j + 2).wait_send()
        return carry

    lax.fori_loop(0, last - 1, drain, 0)


def ring_sum(states, stem, table, ring, mode_rows):
    directions, state_rows, lanes = states.shape
    tiles, stem_rows, depth = stem.shape
    out_rows = 2 * tiles * mode_rows * TILE
    slots = ring + 1
    kept_from = max(2, slots - 15)
    hops = (ring - 1, directions)
    return pl.pallas_call(
        functools.partial(ring_kernel, ring, mode_rows, kept_from),
        out_shape=jax.ShapeDtypeStruct((directions, out_rows, lanes), jnp.float32),
        in_specs=[
            pl.BlockSpec(memory_space=pl.ANY),
            pl.BlockSpec(memory_space=pl.ANY),
            pl.BlockSpec(memory_space=pltpu.VMEM),
        ],
        out_specs=pl.BlockSpec(memory_space=pltpu.VMEM),
        scratch_shapes=[
            pltpu.VMEM((slots, directions, state_rows, lanes), jnp.bfloat16),
            pltpu.VMEM((slots, directions, out_rows, lanes), jnp.bfloat16),
            pltpu.VMEM((slots - kept_from, directions, out_rows, lanes), jnp.float32),
            pltpu.VMEM((2, tiles, stem_rows, depth), jnp.bfloat16),
            pltpu.VMEM((depth, 2 * lanes), jnp.bfloat16),
            pltpu.VMEM((2, stem_rows, 2 * lanes), jnp.float32),
            pltpu.VMEM((table.shape[0], lanes), jnp.float32),
            pltpu.SemaphoreType.DMA((5,)),
            pltpu.SemaphoreType.DMA((2,)),
            pltpu.SemaphoreType.DMA(hops),
            pltpu.SemaphoreType.DMA(hops),
            pltpu.SemaphoreType.DMA(hops),
            pltpu.SemaphoreType.DMA(hops),
        ],
        compiler_params=pltpu.CompilerParams(
            collective_id=0, has_side_effects=True, vmem_limit_bytes=61 * 1024 * 1024
        ),
    )(states, stem, table)


def split(exact):
    upper = lax.reduce_precision(exact, exponent_bits=8, mantissa_bits=7)
    return upper.astype(jnp.bfloat16), (exact - upper).astype(jnp.bfloat16)


def on_device(
    stem_field, first_branch_tensors, second_branch_tensors, relabel, sample_block, sample_state
):
    ring = lax.axis_size("ma")
    groups = ring * lax.axis_size("mb")
    local_blocks, row_count, _, width = stem_field.shape
    mode_rows = row_count // groups
    tiles = groups // TILE
    depth = 2 * width
    block_count = local_blocks * groups
    samples = sample_state.shape[0]
    directions = samples // LANES
    assert lax.axis_size("mb") == 2 and local_blocks == 2 and directions == 2
    assert groups % TILE == 0 and block_count <= 256

    both = jnp.concatenate([first_branch_tensors, second_branch_tensors], axis=0)
    both = lax.all_gather(both, "ma", axis=2, tiled=True)
    rounds = first_branch_tensors.shape[0]
    every_first, every_second = both[:rounds], both[rounds:]

    core = lax.axis_index("mb")
    group = lax.axis_index("ma") * 2 + core
    partner = lax.axis_index("ma") * 2 + 1 - core

    stem = stem_field.reshape(local_blocks, tiles, TILE, mode_rows, depth)
    stem = jnp.transpose(stem, (1, 0, 3, 2, 4)).reshape(row_count * local_blocks, depth)
    inner, outer = complex_table(every_second[0]), complex_table(every_second[1])
    parts = split(jnp.dot(stem, inner, preferred_element_type=jnp.float32))
    stem = sum(jnp.dot(part, outer, preferred_element_type=jnp.float32) for part in parts)
    stem = stem.astype(jnp.bfloat16)
    stem = stem.reshape(tiles, local_blocks * mode_rows * TILE, depth)

    near = jnp.concatenate(
        [group * mode_rows + jnp.arange(mode_rows), partner * mode_rows + jnp.arange(mode_rows)]
    )
    near_hot = (relabel[0][:, None] == near[None, :]).astype(jnp.bfloat16)
    near_rows = jnp.einsum(
        "ij,pio->jpo", near_hot, every_first[0], preferred_element_type=jnp.float32
    ).astype(jnp.bfloat16)
    near_rows = near_rows.reshape(2 * mode_rows, 2, groups, mode_rows)
    table = jnp.transpose(near_rows, (0, 1, 3, 2)).reshape(4 * mode_rows * mode_rows, groups)
    table = jnp.repeat(table, local_blocks, axis=1)
    parity = (jnp.arange(block_count) % local_blocks).astype(jnp.bfloat16)
    table = jnp.concatenate([table, jnp.broadcast_to(parity, (TILE, block_count))], axis=0)

    states = jnp.transpose(sample_state.reshape(directions, LANES, depth), (0, 2, 1))
    named = sample_block.reshape(directions, 1, LANES).astype(jnp.bfloat16)
    states = jnp.concatenate(
        [states, jnp.broadcast_to(named, (directions, TILE, LANES))], axis=1
    )
    summed = ring_sum(states, stem, table, ring, mode_rows)

    order = jnp.arange(row_count).reshape(tiles, TILE, mode_rows)
    order = jnp.transpose(order, (0, 2, 1)).reshape(row_count)
    last_hot = (relabel[1][:, None] == order[None, :]).astype(jnp.bfloat16)
    last = jnp.einsum(
        "ij,pio->pjo", last_hot, every_first[1], preferred_element_type=jnp.float32
    ).astype(jnp.bfloat16)
    final = complex_table(last)
    amplitudes = sum(
        jnp.einsum("dkn,km->dnm", part, final, preferred_element_type=jnp.float32)
        for part in split(summed)
    ).astype(jnp.bfloat16)
    return amplitudes.reshape(samples, 2, last.shape[2])


def solution(mesh):
    placed = (
        P(("cuts", "ma", "mb"), None, None, None),
        P(None, None, "ma", None),
        P(None, None, "ma", None),
        P(),
        P(("cuts", "ma", "mb"), None),
        P(("cuts", "ma", "mb"), None, None),
    )
    return jax.shard_map(
        on_device,
        mesh=mesh,
        in_specs=placed,
        out_specs=P(("cuts", "ma", "mb"), None, None),
        check_vma=False,
    )
```

```python
import functools

import jax
import jax.numpy as jnp
from jax import lax
from jax.experimental import pallas as pl
from jax.experimental.pallas import tpu as pltpu
from jax.sharding import PartitionSpec as P

LANES = 128
TILE = 16
PACE = 3
KEPT = 15
MESH = pl.DeviceIdType.MESH


def complex_table(matrix):
    real_part, imag_part = matrix[0], matrix[1]
    upper_rows = jnp.concatenate([real_part, imag_part], axis=1)
    lower_rows = jnp.concatenate([-imag_part, real_part], axis=1)
    return jnp.concatenate([upper_rows, lower_rows], axis=0)


def spread_kernel(
    ring,
    states_ref,
    shard_ref,
    states,
    gathered,
    local_sem,
    pair_sem,
    state_send,
    state_recv,
    shard_send,
    shard_recv,
):
    me = lax.axis_index("ma")
    core = lax.axis_index("mb")
    right, left = lax.rem(me + 1, ring), lax.rem(me + ring - 1, ring)
    other_core = 1 - core
    hops = ring // 2
    rows = shard_ref.shape[2]
    part = shard_ref.shape[0] // 2

    barrier = pltpu.get_barrier_semaphore()
    pl.semaphore_signal(barrier, inc=1, device_id={"ma": right}, device_id_type=MESH)
    pl.semaphore_signal(barrier, inc=1, device_id={"ma": left}, device_id_type=MESH)
    pl.semaphore_signal(barrier, inc=1, device_id={"mb": other_core}, device_id_type=MESH)

    def held(owner):
        start = pl.multiple_of(owner * rows, rows)
        return gathered.at[pl.ds(core * part, part), :, pl.ds(start, rows), :]

    local = [
        pltpu.make_async_copy(
            states_ref.at[d if j == 0 else 1 - d], states.at[j, d], local_sem.at[2 * j + d]
        )
        for j in range(2)
        for d in range(2)
    ]
    local.append(
        pltpu.make_async_copy(
            shard_ref.at[pl.ds(core * part, part)], held(me), local_sem.at[4]
        )
    )
    for copy in local:
        copy.start()
    pl.semaphore_wait(barrier, 3)
    for copy in local:
        copy.wait()

    def state_copy(d, j):
        return pltpu.make_async_remote_copy(
            src_ref=states.at[j, d],
            dst_ref=states.at[j + 2, d],
            send_sem=state_send.at[j, d],
            recv_sem=state_recv.at[j, d],
            device_id={"ma": (right, left)[d]},
            device_id_type=MESH,
        )

    def shard_copy(d, i, owner):
        return pltpu.make_async_remote_copy(
            src_ref=held(owner),
            dst_ref=held(owner),
            send_sem=shard_send.at[i, d],
            recv_sem=shard_recv.at[i, d],
            device_id={"ma": (right, left)[d]},
            device_id_type=MESH,
        )

    def owner_of(d, i):
        return lax.rem(me + ring - i, ring) if d == 0 else lax.rem(me + i, ring)

    def hop(i, carry):
        for d in range(2):

            @pl.when(i >= 1)
            def _():
                shard_copy(d, i - 1, owner_of(d, i)).wait_recv()

        shard_copy(0, i, owner_of(0, i)).start()

        @pl.when(i < hops - 1)
        def _():
            shard_copy(1, i, owner_of(1, i)).start()

        for d in range(2):

            @pl.when(i >= 2)
            def _():
                state_copy(d, i - 2).wait_recv()

            state_copy(d, i).start()

        return carry

    lax.fori_loop(0, hops, hop, 0)
    shard_copy(0, hops - 1, owner_of(0, hops)).wait_recv()
    mine = gathered.at[pl.ds(core * part, part)]
    pair = pltpu.make_async_remote_copy(
        src_ref=mine,
        dst_ref=mine,
        send_sem=pair_sem.at[0],
        recv_sem=pair_sem.at[1],
        device_id={"mb": other_core},
        device_id_type=MESH,
    )
    pair.start()
    for d in range(2):
        state_copy(d, hops - 2).wait_recv()
        state_copy(d, hops - 1).wait_recv()

    def drain(i, carry):
        for d in range(2):
            state_copy(d, i).wait_send()
        shard_copy(0, i, owner_of(0, i)).wait_send()

        @pl.when(i < hops - 1)
        def _():
            shard_copy(1, i, owner_of(1, i)).wait_send()

        return carry

    lax.fori_loop(0, hops, drain, 0)
    pair.wait()


def first_spread(states, shard, ring):
    directions, state_rows, lanes = states.shape
    tensors, parts, rows, width = shard.shape
    hops = (ring // 2, directions)
    return pl.pallas_call(
        functools.partial(spread_kernel, ring),
        out_shape=(
            jax.ShapeDtypeStruct((ring // 2 + 2, directions, state_rows, lanes), jnp.bfloat16),
            jax.ShapeDtypeStruct((tensors, parts, ring * rows, width), jnp.bfloat16),
        ),
        in_specs=[pl.BlockSpec(memory_space=pl.ANY)] * 2,
        out_specs=(pl.BlockSpec(memory_space=pltpu.VMEM),) * 2,
        scratch_shapes=[
            pltpu.SemaphoreType.DMA((5,)),
            pltpu.SemaphoreType.DMA((2,)),
            pltpu.SemaphoreType.DMA(hops),
            pltpu.SemaphoreType.DMA(hops),
            pltpu.SemaphoreType.DMA(hops),
            pltpu.SemaphoreType.DMA(hops),
        ],
        compiler_params=pltpu.CompilerParams(
            collective_id=1, has_side_effects=True, vmem_limit_bytes=61 * 1024 * 1024
        ),
    )(states, shard)


def ring_kernel(
    ring,
    mode_rows,
    kept_from,
    states_ref,
    stem_ref,
    table_ref,
    out_ref,
    states,
    sums,
    kept,
    stems,
    wide,
    products,
    coef,
    local_sem,
    stem_sem,
    state_send,
    state_recv,
    sum_send,
    sum_recv,
):
    me = lax.axis_index("ma")
    core = lax.axis_index("mb")
    right, left = lax.rem(me + 1, ring), lax.rem(me + ring - 1, ring)
    other_core = 1 - core
    last = ring

    barrier = pltpu.get_barrier_semaphore()
    pl.semaphore_signal(barrier, inc=1, device_id={"ma": right}, device_id_type=MESH)
    pl.semaphore_signal(barrier, inc=1, device_id={"ma": left}, device_id_type=MESH)
    pl.semaphore_signal(barrier, inc=1, device_id={"mb": other_core}, device_id_type=MESH)

    arrived = states_ref.shape[0]
    first = arrived - 2
    own_states = pltpu.make_async_copy(
        states_ref, states.at[pl.ds(0, arrived)], local_sem.at[0]
    )
    own_stem = pltpu.make_async_copy(stem_ref, stems.at[0], local_sem.at[1])
    own_states.start()
    own_stem.start()
    pl.semaphore_wait(barrier, 3)
    swap = pltpu.make_async_remote_copy(
        src_ref=stem_ref,
        dst_ref=stems.at[1],
        send_sem=stem_sem.at[0],
        recv_sem=stem_sem.at[1],
        device_id={"mb": other_core},
        device_id_type=MESH,
    )
    swap.start()
    own_states.wait()

    def state_copy(d, j):
        return pltpu.make_async_remote_copy(
            src_ref=states.at[j, d],
            dst_ref=states.at[j + 2, d],
            send_sem=state_send.at[j - first, d],
            recv_sem=state_recv.at[j - first, d],
            device_id={"ma": (right, left)[d]},
            device_id_type=MESH,
        )

    def sum_copy(d, j):
        return pltpu.make_async_remote_copy(
            src_ref=sums.at[j, d],
            dst_ref=sums.at[j - 2, d],
            send_sem=sum_send.at[j - 2, d],
            recv_sem=sum_recv.at[j - 2, d],
            device_id={"ma": (left, right)[d]},
            device_id_type=MESH,
        )

    tiles = stems.shape[1]
    depth = stems.shape[3]
    half = depth // 2
    blocks = table_ref.shape[1]
    parity_row = 4 * mode_rows * mode_rows
    out_half = tiles * mode_rows * TILE

    def contribution(j, slot):
        def one(d, carry):
            real_part = states[j, d, 0:half, :]
            imag_part = states[j, d, half:depth, :]
            wide[0:half, 0:LANES] = real_part
            wide[0:half, LANES : 2 * LANES] = imag_part
            wide[half:depth, 0:LANES] = -imag_part
            wide[half:depth, LANES : 2 * LANES] = real_part
            named = states[j, d, depth : depth + TILE, :].astype(jnp.float32)[0:1, :]
            counted = lax.broadcasted_iota(jnp.int32, (blocks, LANES), 0).astype(jnp.float32)
            hot = jnp.where(counted == named, 1.0, 0.0).astype(jnp.bfloat16)
            coef[...] = jnp.dot(table_ref[...], hot, preferred_element_type=jnp.float32)

            def tile_step(t, carry):
                for h in range(2):
                    products[h] = jnp.dot(
                        stems[h, t], wide[...], preferred_element_type=jnp.float32
                    )
                odd = jnp.broadcast_to(coef[parity_row : parity_row + 1, :], (TILE, LANES)) > 0.5
                sum_real = [jnp.zeros((TILE, LANES), jnp.float32)] * mode_rows
                sum_imag = [jnp.zeros((TILE, LANES), jnp.float32)] * mode_rows
                for h in range(2):
                    for r in range(mode_rows):
                        even_rows = pl.ds(r * TILE, TILE)
                        odd_rows = pl.ds((mode_rows + r) * TILE, TILE)
                        y_real = jnp.where(
                            odd, products[h, odd_rows, 0:LANES], products[h, even_rows, 0:LANES]
                        )
                        y_imag = jnp.where(
                            odd,
                            products[h, odd_rows, LANES : 2 * LANES],
                            products[h, even_rows, LANES : 2 * LANES],
                        )
                        for q in range(mode_rows):
                            row = ((h * mode_rows + r) * 2) * mode_rows + q
                            c_real = jnp.broadcast_to(coef[row : row + 1, :], (TILE, LANES))
                            row = row + mode_rows
                            c_imag = jnp.broadcast_to(coef[row : row + 1, :], (TILE, LANES))
                            sum_real[q] = sum_real[q] + (c_real * y_real - c_imag * y_imag)
                            sum_imag[q] = sum_imag[q] + (c_real * y_imag + c_imag * y_real)
                for q in range(mode_rows):
                    start = pl.multiple_of(t * (mode_rows * TILE), TILE) + q * TILE
                    kept[slot, d, pl.ds(start, TILE), :] = sum_real[q]
                    kept[slot, d, pl.ds(out_half + start, TILE), :] = sum_imag[q]
                return carry

            return lax.fori_loop(0, tiles, tile_step, carry)

        lax.fori_loop(0, 2, one, 0)

    def spread(j, carry):
        @pl.when(j >= arrived)
        def _():
            for d in range(2):
                state_copy(d, j - 2).wait_recv()

        @pl.when(j <= last - 2)
        def _():
            for d in range(2):
                state_copy(d, j).start()

        @pl.when(j == kept_from)
        def _():
            own_stem.wait()
            swap.wait()

        @pl.when(j >= kept_from)
        def _():
            contribution(j, j - kept_from)

        @pl.when(j >= last - 1)
        def _():
            for d in range(2):
                sums[j, d] = kept[j - kept_from, d].astype(jnp.bfloat16)
                sum_copy(d, j).start()

        return carry

    lax.fori_loop(first, last + 1, spread, 0)
    slots = last + 1 - kept_from

    def collect(i, carry):
        j = last - 2 - i

        for d in range(2):
            sum_copy(d, j + 2).wait_recv()

            @pl.when(jnp.logical_and(j >= 2, j < kept_from))
            def _():
                slot = slots - 1 - lax.rem(kept_from - 1 - j, slots)
                sums[j, d] = (sums[j, d].astype(jnp.float32) + kept[slot, d]).astype(jnp.bfloat16)

            @pl.when(j >= kept_from)
            def _():
                sums[j, d] = (
                    sums[j, d].astype(jnp.float32) + kept[j - kept_from, d]
                ).astype(jnp.bfloat16)

            @pl.when(j >= 2)
            def _():
                sum_copy(d, j).start()

        turn = i - (i + 1) // PACE

        @pl.when(jnp.logical_and(lax.rem(i, PACE) != PACE - 1, turn <= kept_from - 2))
        def _():
            contribution(kept_from - 1 - turn, slots - 1 - lax.rem(turn, slots))

        return carry

    lax.fori_loop(0, last - 1, collect, 0)
    mine = slots - 1 - (kept_from - 2) % slots
    for d in range(2):
        out_ref[d] = (
            sums[0, d].astype(jnp.float32) + sums[1, 1 - d].astype(jnp.float32) + kept[mine, 1 - d]
        )

    def drain(j, carry):
        for d in range(2):

            @pl.when(j >= first)
            def _():
                state_copy(d, j).wait_send()

            sum_copy(d, j + 2).wait_send()
        return carry

    lax.fori_loop(0, last - 1, drain, 0)


def ring_sum(states, stem, table, ring, mode_rows):
    arrived, directions, state_rows, lanes = states.shape
    tiles, stem_rows, depth = stem.shape
    out_rows = 2 * tiles * mode_rows * TILE
    slots = ring + 1
    kept_from = max(arrived, slots - KEPT)
    turns = kept_from - 1
    for turn in range(turns):
        step = (PACE * turn) // (PACE - 1)
        assert step < min(ring - 1, ring - kept_from - 1 + turn)
    hops = (ring - 1, directions)
    left = (ring + 1 - arrived, directions)
    return pl.pallas_call(
        functools.partial(ring_kernel, ring, mode_rows, kept_from),
        out_shape=jax.ShapeDtypeStruct((directions, out_rows, lanes), jnp.float32),
        in_specs=[
            pl.BlockSpec(memory_space=pl.ANY),
            pl.BlockSpec(memory_space=pl.ANY),
            pl.BlockSpec(memory_space=pltpu.VMEM),
        ],
        out_specs=pl.BlockSpec(memory_space=pltpu.VMEM),
        scratch_shapes=[
            pltpu.VMEM((slots, directions, state_rows, lanes), jnp.bfloat16),
            pltpu.VMEM((slots, directions, out_rows, lanes), jnp.bfloat16),
            pltpu.VMEM((slots - kept_from, directions, out_rows, lanes), jnp.float32),
            pltpu.VMEM((2, tiles, stem_rows, depth), jnp.bfloat16),
            pltpu.VMEM((depth, 2 * lanes), jnp.bfloat16),
            pltpu.VMEM((2, stem_rows, 2 * lanes), jnp.float32),
            pltpu.VMEM((table.shape[0], lanes), jnp.float32),
            pltpu.SemaphoreType.DMA((2,)),
            pltpu.SemaphoreType.DMA((2,)),
            pltpu.SemaphoreType.DMA(left),
            pltpu.SemaphoreType.DMA(left),
            pltpu.SemaphoreType.DMA(hops),
            pltpu.SemaphoreType.DMA(hops),
        ],
        compiler_params=pltpu.CompilerParams(
            collective_id=0, has_side_effects=True, vmem_limit_bytes=61 * 1024 * 1024
        ),
    )(states, stem, table)


def split(exact):
    upper = lax.reduce_precision(exact, exponent_bits=8, mantissa_bits=7)
    return upper.astype(jnp.bfloat16), (exact - upper).astype(jnp.bfloat16)


def on_device(
    stem_field, first_branch_tensors, second_branch_tensors, relabel, sample_block, sample_state
):
    ring = lax.axis_size("ma")
    groups = ring * lax.axis_size("mb")
    local_blocks, row_count, _, width = stem_field.shape
    mode_rows = row_count // groups
    tiles = groups // TILE
    depth = 2 * width
    block_count = local_blocks * groups
    samples = sample_state.shape[0]
    directions = samples // LANES
    assert lax.axis_size("mb") == 2 and local_blocks == 2 and directions == 2
    assert groups % TILE == 0 and block_count <= 256

    both = jnp.concatenate([first_branch_tensors, second_branch_tensors], axis=0)
    states = jnp.transpose(sample_state.reshape(directions, LANES, depth), (0, 2, 1))
    named = sample_block.reshape(directions, 1, LANES).astype(jnp.bfloat16)
    states = jnp.concatenate(
        [states, jnp.broadcast_to(named, (directions, TILE, LANES))], axis=1
    )
    states, both = first_spread(states, both, ring)
    rounds = first_branch_tensors.shape[0]
    every_first, every_second = both[:rounds], both[rounds:]

    core = lax.axis_index("mb")
    group = lax.axis_index("ma") * 2 + core
    partner = lax.axis_index("ma") * 2 + 1 - core

    stem = stem_field.reshape(local_blocks, tiles, TILE, mode_rows, depth)
    stem = jnp.transpose(stem, (1, 0, 3, 2, 4)).reshape(row_count * local_blocks, depth)
    inner, outer = complex_table(every_second[0]), complex_table(every_second[1])
    parts = split(jnp.dot(stem, inner, preferred_element_type=jnp.float32))
    stem = sum(jnp.dot(part, outer, preferred_element_type=jnp.float32) for part in parts)
    stem = stem.astype(jnp.bfloat16)
    stem = stem.reshape(tiles, local_blocks * mode_rows * TILE, depth)

    near = jnp.concatenate(
        [group * mode_rows + jnp.arange(mode_rows), partner * mode_rows + jnp.arange(mode_rows)]
    )
    near_hot = (relabel[0][:, None] == near[None, :]).astype(jnp.bfloat16)
    near_rows = jnp.einsum(
        "ij,pio->jpo", near_hot, every_first[0], preferred_element_type=jnp.float32
    ).astype(jnp.bfloat16)
    near_rows = near_rows.reshape(2 * mode_rows, 2, groups, mode_rows)
    table = jnp.transpose(near_rows, (0, 1, 3, 2)).reshape(4 * mode_rows * mode_rows, groups)
    table = jnp.repeat(table, local_blocks, axis=1)
    parity = (jnp.arange(block_count) % local_blocks).astype(jnp.bfloat16)
    table = jnp.concatenate([table, jnp.broadcast_to(parity, (TILE, block_count))], axis=0)

    summed = ring_sum(states, stem, table, ring, mode_rows)

    order = jnp.arange(row_count).reshape(tiles, TILE, mode_rows)
    order = jnp.transpose(order, (0, 2, 1)).reshape(row_count)
    last_hot = (relabel[1][:, None] == order[None, :]).astype(jnp.bfloat16)
    last = jnp.einsum(
        "ij,pio->pjo", last_hot, every_first[1], preferred_element_type=jnp.float32
    ).astype(jnp.bfloat16)
    final = complex_table(last)
    amplitudes = sum(
        jnp.einsum("dkn,km->dnm", part, final, preferred_element_type=jnp.float32)
        for part in split(summed)
    ).astype(jnp.bfloat16)
    return amplitudes.reshape(samples, 2, last.shape[2])


def solution(mesh):
    placed = (
        P(("cuts", "ma", "mb"), None, None, None),
        P(None, None, "ma", None),
        P(None, None, "ma", None),
        P(),
        P(("cuts", "ma", "mb"), None),
        P(("cuts", "ma", "mb"), None, None),
    )
    return jax.shard_map(
        on_device,
        mesh=mesh,
        in_specs=placed,
        out_specs=P(("cuts", "ma", "mb"), None, None),
        check_vma=False,
    )
```
